32 devices in a mesh: expert: 8 (over z, core), mp: 4 (over y, x).
Axes of the slice: x: 2, y: 2, z: 4, core: 2. Of those that a mesh axis runs over, the one named last changes fastest.
Arguments:
- tokens: bfloat16 [2, 2560, 2048], P(None, 'expert', 'mp'), may hold values from -6 to 6
- expert_index: int32 [2, 2560], P(None, 'expert'), may hold values from 0 to 7
- slot_index: int32 [2, 2560], P(None, 'expert'), may hold values from 0 to 5, as said below
- kept_mask: int32 [2, 2560], P(None, 'expert'), may hold values from 0 to 1
- gate_prob: float32 [2, 2560], P(None, 'expert'), may hold values from 0.2 to 1
- w_in: bfloat16 [8, 2048, 6144], P('expert', None, 'mp'), may hold values from -0.125 to 0.125
- w_out: bfloat16 [8, 6144, 2048], P('expert', 'mp'), may hold values from -0.078125 to 0.078125
Outputs:
- mixed: bfloat16 [2, 2560, 2048], P(None, 'expert', 'mp')
The draws below stay inside these ranges and needn't reach their ends.
Inputs may be any that keep to these rules, and one draw needn't show every extreme that they name: `slot_index`: within one aligned block of 320 tokens of a group, no two kept tokens share both expert and slot; in every group some expert has all 6 slots of every block taken. Dropped tokens carry a slot value too, which means nothing.
All inputs are finite; a program needn't handle non-finite values.
Results may differ from the reference program's by a relative error of at most 0.018.
Values may be sent and summed in bfloat16 or wider, within the bound.
A program may use at most 64 MiB of HBM per device.

```python
import jax
import jax.numpy as jnp
from jax import lax

D = 2048
FF = 6144
GROUPS = 2
TOK_GRP = 320
CAP = 6
EXPERTS = 8
TOKENS = 2560
N_EXPERT = 8
N_MP = 4


def routing(key):
    base = jax.random.fold_in(key, 7)
    first_key, second_key, third_key = jax.random.split(base, 3)
    blocks = GROUPS * (TOKENS // TOK_GRP)
    favored = jax.random.randint(first_key, (GROUPS, 1), 0, EXPERTS)
    favored = jnp.repeat(favored, TOKENS // TOK_GRP, axis=0)
    picks = jax.random.randint(second_key, (blocks, TOK_GRP), 0, EXPERTS)
    scores = jax.random.randint(third_key, (blocks, TOK_GRP), 0, 2 ** 20)
    scores = scores * TOK_GRP + jnp.arange(TOK_GRP, dtype=jnp.int32)[None, :]
    ranking = jnp.argsort(jnp.argsort(scores, axis=1), axis=1)
    chosen = jnp.where(ranking < 2 * CAP, favored, picks).astype(jnp.int32)
    onehot = (chosen[:, :, None] == jnp.arange(EXPERTS, dtype=jnp.int32)[None, None, :]).astype(jnp.int32)
    before = jnp.cumsum(onehot, axis=1) - onehot
    position = jnp.sum(before * onehot, axis=2)
    kept = (position < CAP).astype(jnp.int32)
    slot = (position % CAP).astype(jnp.int32)
    return (chosen.reshape(GROUPS, TOKENS), slot.reshape(GROUPS, TOKENS), kept.reshape(GROUPS, TOKENS))


def draw_expert_index(key, part):
    return routing(key)[0]


def draw_slot_index(key, part):
    return routing(key)[1]


def draw_kept_mask(key, part):
    return routing(key)[2]


def block_levels(rng, dims, pieces, low, high):
    def one(dim, shards_of):
        steps = jax.random.uniform(jax.random.fold_in(jax.random.fold_in(rng, 6), dim), (shards_of,), jnp.float32, low / len(pieces), high / len(pieces))
        return jnp.repeat(jnp.exp(steps), dims[dim] // shards_of).reshape((-1,) + (1,) * (len(dims) - dim - 1))

    gain = one(*pieces[0])
    for cut in pieces[1:]:
        gain = gain * one(*cut)
    return gain


def centred(stream_key, dims, scale, bound, shards=(), held_as=jnp.bfloat16):
    entries = jax.random.normal(stream_key, dims, jnp.float32) * scale
    if len(shards) > 0:
        entries = block_levels(stream_key, dims, shards, -0.22, 0.18) * entries
    return jnp.clip(entries, min=-bound, max=bound).astype(held_as)


def setup_inputs(seed: int = 0) -> dict:
    seeds = jax.random.split(jax.random.key(seed), 8)
    tokens = centred(seeds[0], (GROUPS, TOKENS, D), 1.0, 6.0, ((1, 8), (2, 4)))
    expert_index = draw_expert_index(jax.random.fold_in(seeds[7], 71), 0)
    slot_index = draw_slot_index(jax.random.fold_in(seeds[7], 71), 0)
    kept_mask = draw_kept_mask(jax.random.fold_in(seeds[7], 71), 0)
    gate_prob = jnp.clip(0.2 + 0.8 * jax.random.uniform(seeds[4], (GROUPS, TOKENS), jnp.float32) ** block_levels(seeds[4], (GROUPS, TOKENS), ((1, 8),), -0.2, 0.2), 0.2, 1.0)
    w_in = centred(seeds[5], (EXPERTS, D, FF), D ** -0.5, 0.125, ((0, 8), (2, 4)))
    w_out = centred(seeds[6], (EXPERTS, FF, D), FF ** -0.5, 0.078125, ((0, 8), (1, 4)))
    return dict(tokens=tokens, expert_index=expert_index, slot_index=slot_index, kept_mask=kept_mask, gate_prob=gate_prob, w_in=w_in, w_out=w_out)


def reference(tokens, expert_index, slot_index, kept_mask, gate_prob, w_in, w_out):
    rows_each = N_EXPERT * CAP
    width = FF // N_MP
    source = (jnp.arange(TOKENS, dtype=jnp.int32) // TOK_GRP).astype(jnp.int32)

    def expert_work(args):
        block, first, second = args
        pre = jnp.dot(block, first, preferred_element_type=jnp.float32)
        hidden = jnp.maximum(pre, 0.0).astype(jnp.bfloat16)
        total = jnp.zeros((rows_each, D), jnp.float32)
        for k in range(N_MP):
            part = jnp.dot(hidden[:, k * width:(k + 1) * width], second[k * width:(k + 1) * width],
                           preferred_element_type=jnp.float32).astype(jnp.bfloat16)
            part = lax.optimization_barrier(part)
            total = total + part.astype(jnp.float32)
        return total.astype(jnp.bfloat16)

    results = []
    for group in range(GROUPS):
        place = expert_index[group] * rows_each + source * CAP + slot_index[group]
        place = jnp.where(kept_mask[group] > 0, place, EXPERTS * rows_each).astype(jnp.int32)
        buffer = jnp.zeros((EXPERTS * rows_each + 1, D), jnp.bfloat16).at[place].set(tokens[group])
        buffer = buffer[:-1].reshape(EXPERTS, rows_each, D)
        done = lax.map(expert_work, (buffer, w_in, w_out)).reshape(EXPERTS * rows_each, D)
        picked = done[jnp.minimum(place, EXPERTS * rows_each - 1).astype(jnp.int32)].astype(jnp.float32)
        mixed = jnp.where(kept_mask[group][:, None] > 0, gate_prob[group][:, None] * picked, 0.0)
        results.append(mixed.astype(jnp.bfloat16))
    return jnp.stack(results)
```

```python
import functools

import jax
import jax.numpy as jnp
from jax import lax
from jax.experimental import pallas as pl
from jax.experimental.pallas import tpu as pltpu
from jax.sharding import PartitionSpec as P

GROUPS = 2
CAP = 6
SLOTS = -(-GROUPS * CAP // 16) * 16
MESH = pl.DeviceIdType.MESH


def flip(index, k):
    out = index
    bit = 1
    while bit <= k:
        if k & bit:
            out = out + bit - 2 * bit * ((index // bit) % 2)
        bit *= 2
    return out


def rows_of(index, size):
    return pl.ds(pl.multiple_of(index * size, size), size)


def places(index, slot, kept, group):
    return jnp.where(kept > 0, index * SLOTS + group * CAP + slot, -1)


def expert_kernel(
    experts, mp, pieces,
    index_ref, slot_ref, kept_ref, tokens_hbm, w_in_hbm, w_out_hbm, out_hbm,
    tokens, first, second, packed, gathered, pre, hidden, partial, arrived, outgoing, returned,
    token_sem, first_sem, second_sem, own_sem,
    a_send, a_recv, g_send, g_recv, r_send, r_recv, b_send, b_recv, out_sem,
):
    me = lax.axis_index("expert")
    col = lax.axis_index("mp")
    narrow = tokens.shape[2]
    each = experts // pieces
    span = each * SLOTS
    mine = me // each

    def remote(src, dst, send, recv, expert, column):
        return pltpu.make_async_remote_copy(
            src_ref=src, dst_ref=dst, send_sem=send, recv_sem=recv,
            device_id=(expert, column), device_id_type=MESH,
        )

    barrier = pltpu.get_barrier_semaphore()
    for j in range(1, experts):
        pl.semaphore_signal(barrier, inc=1, device_id=(flip(me, j), col), device_id_type=MESH)
    for k in range(1, mp):
        pl.semaphore_signal(barrier, inc=1, device_id=(me, flip(col, k)), device_id_type=MESH)

    token_copy = pltpu.make_async_copy(tokens_hbm, tokens, token_sem)
    token_copy.start()
    first_copies = []
    for k in range(mp):
        m = flip(col, k)
        copy = pltpu.make_async_copy(
            w_in_hbm.at[0, rows_of(m, narrow), :], first.at[m], first_sem.at[k]
        )
        copy.start()
        first_copies.append(copy)
    out_order = list(range(mp - 1, -1, -1))
    second_copies = {}
    for k in out_order:
        m = flip(col, k)
        copy = pltpu.make_async_copy(
            w_out_hbm.at[0, :, rows_of(m, narrow)], second.at[m], second_sem.at[k]
        )
        copy.start()
        second_copies[k] = copy

    token_copy.wait()
    total = jnp.zeros((experts * SLOTS, narrow), jnp.float32)
    for group in range(GROUPS):
        code = places(
            index_ref[pl.ds(group, 1), :], slot_ref[pl.ds(group, 1), :],
            kept_ref[pl.ds(group, 1), :], group,
        )
        rows = lax.broadcasted_iota(jnp.int32, (experts * SLOTS, code.shape[1]), 0)
        table = jnp.where(rows == code, 1.0, 0.0).astype(jnp.bfloat16)
        total = total + jnp.dot(table, tokens[group], preferred_element_type=jnp.float32)
    packed[...] = total.astype(jnp.bfloat16)

    pl.semaphore_wait(barrier, experts + mp - 2)

    own = pltpu.make_async_copy(
        packed.at[rows_of(me, SLOTS), :], gathered.at[col, rows_of(me, SLOTS), :], own_sem
    )
    own.start()

    def exchange(j):
        e = flip(me, j)
        return remote(
            packed.at[rows_of(e, SLOTS), :], gathered.at[col, rows_of(me, SLOTS), :],
            a_send.at[j], a_recv.at[j], e, col,
        )

    def exchange_arrival(j):
        e = flip(me, j)
        return remote(
            packed.at[rows_of(e, SLOTS), :], gathered.at[col, rows_of(e, SLOTS), :],
            a_send.at[j], a_recv.at[j], e, col,
        )

    for j in list(range(1, each)) + list(range(experts - 1, each - 1, -1)):
        exchange(j).start()

    def gather(k, q, owner):
        block = gathered.at[owner, rows_of(flip(mine, q), span), :]
        return remote(block, block, g_send.at[k, q], g_recv.at[k, q], me, flip(col, k))

    for q in range(pieces):
        for j in range(q * each, (q + 1) * each):
            if j == 0:
                own.wait()
            else:
                exchange_arrival(j).wait_recv()
        for k in range(mp - 1, 0, -1):
            gather(k, q, col).start()

    for k in range(mp):
        m = flip(col, k)
        first_copies[k].wait()
        if k > 0:
            for q in range(pieces):
                gather(k, q, m).wait_recv()
        product = jnp.dot(gathered[m], first[m], preferred_element_type=jnp.float32)
        if k == 0:
            pre[...] = product
        elif k < mp - 1:
            pre[...] += product
        else:
            hidden[...] = jnp.maximum(pre[...] + product, 0.0).astype(jnp.bfloat16)

    def scatter(k, q, sender):
        rows = rows_of(flip(mine, q), span)
        return remote(
            partial.at[flip(col, k), rows, :], arrived.at[sender, rows, :],
            r_send.at[k, q], r_recv.at[k, q], me, flip(col, k),
        )

    for k in out_order:
        m = flip(col, k)
        second_copies[k].wait()
        partial[m] = jnp.dot(
            hidden[...], second[m], preferred_element_type=jnp.float32
        ).astype(jnp.bfloat16)
        if k > 0:
            for q in range(pieces - 1, -1, -1):
                scatter(k, q, col).start()

    def give_back(j):
        e = flip(me, j)
        return remote(
            outgoing.at[rows_of(e, SLOTS), :], returned.at[rows_of(me, SLOTS), :],
            b_send.at[j], b_recv.at[j], e, col,
        )

    def give_back_arrival(j):
        e = flip(me, j)
        return remote(
            outgoing.at[rows_of(e, SLOTS), :], returned.at[rows_of(e, SLOTS), :],
            b_send.at[j], b_recv.at[j], e, col,
        )

    for q in range(pieces - 1, -1, -1):
        rows = rows_of(flip(mine, q), span)
        summed = partial[col, rows, :].astype(jnp.float32)
        for k in range(1, mp):
            m = flip(col, k)
            scatter(k, q, m).wait_recv()
            summed = summed + arrived[m, rows, :].astype(jnp.float32)
        outgoing[rows, :] = summed.astype(jnp.bfloat16)
        for j in range((q + 1) * each - 1, q * each - 1, -1):
            if j > 0:
                give_back(j).start()
            else:
                own_back = pltpu.make_async_copy(
                    outgoing.at[rows_of(me, SLOTS), :], returned.at[rows_of(me, SLOTS), :], own_sem
                )
                own_back.start()

    own_back.wait()
    for j in range(1, experts):
        give_back_arrival(j).wait_recv()
    result = pltpu.make_async_copy(returned, out_hbm, out_sem)
    result.start()
    for j in range(1, experts):
        exchange(j).wait_send()
        give_back(j).wait_send()
    for k in range(1, mp):
        for q in range(pieces):
            gather(k, q, col).wait_send()
            scatter(k, q, col).wait_send()
    result.wait()


def combine_kernel(index_ref, slot_ref, kept_ref, gate_ref, returned_ref, out_ref):
    held = index_ref.shape[1]
    diagonal = lax.broadcasted_iota(jnp.int32, (held, held), 0) == lax.broadcasted_iota(
        jnp.int32, (held, held), 1
    )
    for group in range(GROUPS):
        code = places(
            index_ref[pl.ds(group, 1), :], slot_ref[pl.ds(group, 1), :],
            kept_ref[pl.ds(group, 1), :], group,
        ).astype(jnp.float32)
        code = jnp.sum(jnp.where(diagonal, code, 0.0), axis=1, keepdims=True)
        gate = jnp.sum(
            jnp.where(diagonal, gate_ref[pl.ds(group, 1), :], 0.0), axis=1, keepdims=True
        )
        lanes = lax.broadcasted_iota(jnp.int32, (held, returned_ref.shape[0]), 1)
        table = jnp.where(lanes == code.astype(jnp.int32), 1.0, 0.0).astype(jnp.bfloat16)
        picked = jnp.dot(table, returned_ref[...], preferred_element_type=jnp.float32)
        out_ref[group] = (gate * picked).astype(jnp.bfloat16)


def on_device(experts, mp, tokens, expert_index, slot_index, kept_mask, gate_prob, w_in, w_out):
    narrow = tokens.shape[2]
    width = w_in.shape[2]
    rows = experts * SLOTS
    pieces = max(1, min(experts, 8) // 2)
    vmem = pl.BlockSpec(memory_space=pltpu.VMEM)
    hbm = pl.BlockSpec(memory_space=pl.ANY)
    dma = pltpu.SemaphoreType.DMA
    bf16 = jnp.bfloat16
    returned = pl.pallas_call(
        functools.partial(expert_kernel, experts, mp, pieces),
        out_shape=jax.ShapeDtypeStruct((rows, narrow), bf16),
        in_specs=[vmem] * 3 + [hbm] * 3,
        out_specs=hbm,
        scratch_shapes=[
            pltpu.VMEM(tokens.shape, bf16),
            pltpu.VMEM((mp, narrow, width), bf16),
            pltpu.VMEM((mp, width, narrow), bf16),
            pltpu.VMEM((rows, narrow), bf16),
            pltpu.VMEM((mp, rows, narrow), bf16),
            pltpu.VMEM((rows, width), jnp.float32),
            pltpu.VMEM((rows, width), bf16),
            pltpu.VMEM((mp, rows, narrow), bf16),
            pltpu.VMEM((mp, rows, narrow), bf16),
            pltpu.VMEM((rows, narrow), bf16),
            pltpu.VMEM((rows, narrow), bf16),
            dma, dma((mp,)), dma((mp,)), dma,
            dma((experts,)), dma((experts,)),
            dma((mp, pieces)), dma((mp, pieces)),
            dma((mp, pieces)), dma((mp, pieces)),
            dma((experts,)), dma((experts,)),
            dma,
        ],
        compiler_params=pltpu.CompilerParams(
            collective_id=0, has_side_effects=True, vmem_limit_bytes=60000 * 1024
        ),
    )(expert_index, slot_index, kept_mask, tokens, w_in, w_out)
    return pl.pallas_call(
        combine_kernel,
        out_shape=jax.ShapeDtypeStruct(tokens.shape, bf16),
        in_specs=[vmem] * 5,
        out_specs=vmem,
    )(expert_index, slot_index, kept_mask, gate_prob, returned)


def solution(mesh):
    placed = (
        P(None, "expert", "mp"),
        P(None, "expert"),
        P(None, "expert"),
        P(None, "expert"),
        P(None, "expert"),
        P("expert", None, "mp"),
        P("expert", "mp", None),
    )
    return jax.shard_map(
        functools.partial(on_device, mesh.shape["expert"], mesh.shape["mp"]),
        mesh=mesh, in_specs=placed, out_specs=P(None, "expert", "mp"), check_vma=False,
    )
```

```python
import functools

import jax
import jax.numpy as jnp
from jax import lax
from jax.experimental import pallas as pl
from jax.experimental.pallas import tpu as pltpu
from jax.sharding import PartitionSpec as P

GROUPS = 2
CAP = 6
SLOTS = -(-GROUPS * CAP // 16) * 16
USED = GROUPS * CAP
HALVES = 2
MESH = pl.DeviceIdType.MESH


def flip(index, k):
    out = index
    bit = 1
    while bit <= k:
        if k & bit:
            out = out + bit - 2 * bit * ((index // bit) % 2)
        bit *= 2
    return out


def rows_of(index, size):
    return pl.ds(pl.multiple_of(index * size, size), size)


def compact_table(rows, padded, transposed):
    shape = (padded, rows) if transposed else (rows, padded)
    wide = lax.broadcasted_iota(jnp.int32, shape, 0 if transposed else 1)
    slim = lax.broadcasted_iota(jnp.int32, shape, 1 if transposed else 0)
    within = lax.rem(wide, SLOTS)
    match = (lax.div(wide, SLOTS) * USED + within == slim) & (within < USED)
    return jnp.where(match, 1.0, 0.0).astype(jnp.bfloat16)


def places(index, slot, kept, group):
    return jnp.where(kept > 0, index * SLOTS + group * CAP + slot, -1)


def expert_kernel(
    experts, mp,
    index_ref, slot_ref, kept_ref, tokens_hbm, w_in_hbm, w_out_hbm, out_hbm,
    tokens, first, second, packed, inbox, gathered, pre, hidden, partial, arrived, outgoing, returned,
    token_sem, first_sem, second_sem,
    a_send, a_recv, g_send, g_recv, r_send, r_recv, b_send, b_recv, out_sem,
):
    me = lax.axis_index("expert")
    col = lax.axis_index("mp")
    narrow = tokens.shape[2]
    each = experts // HALVES
    span = each * SLOTS
    slim = each * USED
    mine = me // each

    def remote(src, dst, send, recv, expert, column):
        return pltpu.make_async_remote_copy(
            src_ref=src, dst_ref=dst, send_sem=send, recv_sem=recv,
            device_id=(expert, column), device_id_type=MESH,
        )

    barrier = pltpu.get_barrier_semaphore()
    for j in range(1, experts):
        pl.semaphore_signal(barrier, inc=1, device_id=(flip(me, j), col), device_id_type=MESH)
    for k in range(1, mp):
        pl.semaphore_signal(barrier, inc=1, device_id=(me, flip(col, k)), device_id_type=MESH)

    token_copy = pltpu.make_async_copy(tokens_hbm, tokens, token_sem)
    token_copy.start()
    first_copies = []
    for k in range(mp):
        m = flip(col, k)
        copy = pltpu.make_async_copy(
            w_in_hbm.at[0, rows_of(m, narrow), :], first.at[m], first_sem.at[k]
        )
        copy.start()
        first_copies.append(copy)
    out_order = list(range(mp - 1, -1, -1))
    second_copies = {}
    for k in out_order:
        m = flip(col, k)
        copy = pltpu.make_async_copy(
            w_out_hbm.at[0, :, rows_of(m, narrow)], second.at[m], second_sem.at[k]
        )
        copy.start()
        second_copies[k] = copy

    token_copy.wait()
    total = jnp.zeros((experts * SLOTS, narrow), jnp.float32)
    for group in range(GROUPS):
        code = places(
            index_ref[pl.ds(group, 1), :], slot_ref[pl.ds(group, 1), :],
            kept_ref[pl.ds(group, 1), :], group,
        )
        rows = lax.broadcasted_iota(jnp.int32, (experts * SLOTS, code.shape[1]), 0)
        table = jnp.where(rows == code, 1.0, 0.0).astype(jnp.bfloat16)
        total = total + jnp.dot(table, tokens[group], preferred_element_type=jnp.float32)
    packed[...] = total.astype(jnp.bfloat16)

    pl.semaphore_wait(barrier, experts + mp - 2)

    def exchange(j):
        e = flip(me, j)
        return remote(
            packed.at[rows_of(e, SLOTS), :], inbox.at[rows_of(me, SLOTS), :],
            a_send.at[j], a_recv.at[j], e, col,
        )

    def exchange_arrival(j):
        e = flip(me, j)
        return remote(
            packed.at[rows_of(e, SLOTS), :], inbox.at[rows_of(e, SLOTS), :],
            a_send.at[j], a_recv.at[j], e, col,
        )

    for j in range(experts - 1, 0, -1):
        exchange(j).start()
    inbox[rows_of(me, SLOTS), :] = packed[rows_of(me, SLOTS), :]

    def gather(k, h, owner):
        block = gathered.at[owner, rows_of(flip(mine, h), slim), :]
        return remote(block, block, g_send.at[k, h], g_recv.at[k, h], me, flip(col, k))

    def spread(h):
        for j in range(h * each, (h + 1) * each):
            if j > 0:
                exchange_arrival(j).wait_recv()
        half = flip(mine, h)
        table = compact_table(slim, span, False)
        gathered[col, rows_of(half, slim), :] = jnp.dot(
            table, inbox[rows_of(half, span), :], preferred_element_type=jnp.float32
        ).astype(jnp.bfloat16)
        for k in range(mp - 1, 0, -1):
            gather(k, h, col).start()

    def first_product(h, k):
        m = flip(col, k)
        if h == 0:
            first_copies[k].wait()
        if k > 0:
            gather(k, h, m).wait_recv()
        product = jnp.dot(
            gathered[m, rows_of(flip(mine, h), slim), :], first[m],
            preferred_element_type=jnp.float32,
        )
        if k == 0:
            pre[h] = product
        elif k < mp - 1:
            pre[h] += product
        else:
            hidden[...] = jnp.maximum(pre[h] + product, 0.0).astype(jnp.bfloat16)

    def scatter(k, h, sender):
        rows = rows_of(flip(mine, h), slim)
        return remote(
            partial.at[flip(col, k), rows, :], arrived.at[sender, rows, :],
            r_send.at[k, h], r_recv.at[k, h], me, flip(col, k),
        )

    def second_products(h):
        for k in out_order:
            m = flip(col, k)
            if h == 0:
                second_copies[k].wait()
            partial[m, rows_of(flip(mine, h), slim), :] = jnp.dot(
                hidden[...], second[m], preferred_element_type=jnp.float32
            ).astype(jnp.bfloat16)
            if k > 0:
                scatter(k, h, col).start()

    for h in range(HALVES):
        spread(h)
        first_product(h, 0)
    for h in range(HALVES):
        for k in range(1, mp):
            first_product(h, k)
        second_products(h)

    def give_back(j):
        e = flip(me, j)
        return remote(
            outgoing.at[rows_of(e, SLOTS), :], returned.at[rows_of(me, SLOTS), :],
            b_send.at[j], b_recv.at[j], e, col,
        )

    def give_back_arrival(j):
        e = flip(me, j)
        return remote(
            outgoing.at[rows_of(e, SLOTS), :], returned.at[rows_of(e, SLOTS), :],
            b_send.at[j], b_recv.at[j], e, col,
        )

    for h in range(HALVES):
        half = flip(mine, h)
        rows = rows_of(half, slim)
        summed = partial[col, rows, :].astype(jnp.float32)
        for k in range(1, mp):
            m = flip(col, k)
            scatter(k, h, m).wait_recv()
            summed = summed + arrived[m, rows, :].astype(jnp.float32)
        table = compact_table(slim, span, True)
        outgoing[rows_of(half, span), :] = jnp.dot(
            table, summed.astype(jnp.bfloat16), preferred_element_type=jnp.float32
        ).astype(jnp.bfloat16)
        for j in range((h + 1) * each - 1, h * each - 1, -1):
            if j > 0:
                give_back(j).start()
    returned[rows_of(me, SLOTS), :] = outgoing[rows_of(me, SLOTS), :]
    for j in range(1, experts):
        give_back_arrival(j).wait_recv()
    result = pltpu.make_async_copy(returned, out_hbm, out_sem)
    result.start()
    for j in range(1, experts):
        exchange(j).wait_send()
        give_back(j).wait_send()
    for k in range(1, mp):
        for h in range(HALVES):
            gather(k, h, col).wait_send()
            scatter(k, h, col).wait_send()
    result.wait()


def combine_kernel(index_ref, slot_ref, kept_ref, gate_ref, returned_ref, out_ref):
    held = index_ref.shape[1]
    diagonal = lax.broadcasted_iota(jnp.int32, (held, held), 0) == lax.broadcasted_iota(
        jnp.int32, (held, held), 1
    )
    for group in range(GROUPS):
        code = places(
            index_ref[pl.ds(group, 1), :], slot_ref[pl.ds(group, 1), :],
            kept_ref[pl.ds(group, 1), :], group,
        ).astype(jnp.float32)
        code = jnp.sum(jnp.where(diagonal, code, 0.0), axis=1, keepdims=True)
        gate = jnp.sum(
            jnp.where(diagonal, gate_ref[pl.ds(group, 1), :], 0.0), axis=1, keepdims=True
        )
        lanes = lax.broadcasted_iota(jnp.int32, (held, returned_ref.shape[0]), 1)
        table = jnp.where(lanes == code.astype(jnp.int32), 1.0, 0.0).astype(jnp.bfloat16)
        picked = jnp.dot(table, returned_ref[...], preferred_element_type=jnp.float32)
        out_ref[group] = (gate * picked).astype(jnp.bfloat16)


def on_device(experts, mp, tokens, expert_index, slot_index, kept_mask, gate_prob, w_in, w_out):
    narrow = tokens.shape[2]
    width = w_in.shape[2]
    rows = experts * SLOTS
    slim = experts * USED
    vmem = pl.BlockSpec(memory_space=pltpu.VMEM)
    hbm = pl.BlockSpec(memory_space=pl.ANY)
    dma = pltpu.SemaphoreType.DMA
    bf16 = jnp.bfloat16
    returned = pl.pallas_call(
        functools.partial(expert_kernel, experts, mp),
        out_shape=jax.ShapeDtypeStruct((rows, narrow), bf16),
        in_specs=[vmem] * 3 + [hbm] * 3,
        out_specs=hbm,
        scratch_shapes=[
            pltpu.VMEM(tokens.shape, bf16),
            pltpu.VMEM((mp, narrow, width), bf16),
            pltpu.VMEM((mp, width, narrow), bf16),
            pltpu.VMEM((rows, narrow), bf16),
            pltpu.VMEM((rows, narrow), bf16),
            pltpu.VMEM((mp, slim, narrow), bf16),
            pltpu.VMEM((HALVES, slim // HALVES, width), jnp.float32),
            pltpu.VMEM((slim // HALVES, width), bf16),
            pltpu.VMEM((mp, slim, narrow), bf16),
            pltpu.VMEM((mp, slim, narrow), bf16),
            pltpu.VMEM((rows, narrow), bf16),
            pltpu.VMEM((rows, narrow), bf16),
            dma, dma((mp,)), dma((mp,)),
            dma((experts,)), dma((experts,)),
            dma((mp, HALVES)), dma((mp, HALVES)),
            dma((mp, HALVES)), dma((mp, HALVES)),
            dma((experts,)), dma((experts,)),
            dma,
        ],
        compiler_params=pltpu.CompilerParams(
            collective_id=0, has_side_effects=True, vmem_limit_bytes=60000 * 1024
        ),
    )(expert_index, slot_index, kept_mask, tokens, w_in, w_out)
    return pl.pallas_call(
        combine_kernel,
        out_shape=jax.ShapeDtypeStruct(tokens.shape, bf16),
        in_specs=[vmem] * 5,
        out_specs=vmem,
    )(expert_index, slot_index, kept_mask, gate_prob, returned)


def solution(mesh):
    placed = (
        P(None, "expert", "mp"),
        P(None, "expert"),
        P(None, "expert"),
        P(None, "expert"),
        P(None, "expert"),
        P("expert", None, "mp"),
        P("expert", "mp", None),
    )
    return jax.shard_map(
        functools.partial(on_device, mesh.shape["expert"], mesh.shape["mp"]),
        mesh=mesh, in_specs=placed, out_specs=P(None, "expert", "mp"), check_vma=False,
    )
```

```python
import functools

import jax
import jax.numpy as jnp
from jax import lax
from jax.experimental import pallas as pl
from jax.experimental.pallas import tpu as pltpu
from jax.sharding import PartitionSpec as P

GROUPS = 2
CAP = 6
SLOTS = -(-GROUPS * CAP // 16) * 16
USED = GROUPS * CAP
HALVES = 2
MESH = pl.DeviceIdType.MESH


def flip(index, k):
    out = index
    bit = 1
    while bit <= k:
        if k & bit:
            out = out + bit - 2 * bit * ((index // bit) % 2)
        bit *= 2
    return out


def rows_of(index, size):
    return pl.ds(pl.multiple_of(index * size, size), size)


def compact_table(rows, padded, transposed):
    shape = (padded, rows) if transposed else (rows, padded)
    wide = lax.broadcasted_iota(jnp.int32, shape, 0 if transposed else 1)
    slim = lax.broadcasted_iota(jnp.int32, shape, 1 if transposed else 0)
    within = lax.rem(wide, SLOTS)
    match = (lax.div(wide, SLOTS) * USED + within == slim) & (within < USED)
    return jnp.where(match, 1.0, 0.0).astype(jnp.bfloat16)


def places(index, slot, kept, group):
    return jnp.where(kept > 0, index * SLOTS + group * CAP + slot, -1)


def expert_kernel(
    experts, mp,
    index_ref, slot_ref, kept_ref, tokens_hbm, w_in_hbm, w_out_hbm, out_hbm,
    tokens, first, second, packed, inbox, gathered, pre, hidden, partial, arrived, outgoing, returned,
    token_sem, first_sem, second_sem,
    a_send, a_recv, g_send, g_recv, r_send, r_recv, b_send, b_recv, out_sem,
):
    me = lax.axis_index("expert")
    col = lax.axis_index("mp")
    narrow = tokens.shape[2]
    each = experts // HALVES
    span = each * SLOTS
    slim = each * USED
    mine = me // each

    def remote(src, dst, send, recv, expert, column):
        return pltpu.make_async_remote_copy(
            src_ref=src, dst_ref=dst, send_sem=send, recv_sem=recv,
            device_id=(expert, column), device_id_type=MESH,
        )

    barrier = pltpu.get_barrier_semaphore()
    for j in range(1, experts):
        pl.semaphore_signal(barrier, inc=1, device_id=(flip(me, j), col), device_id_type=MESH)
    for k in range(1, mp):
        pl.semaphore_signal(barrier, inc=1, device_id=(me, flip(col, k)), device_id_type=MESH)

    token_copy = pltpu.make_async_copy(tokens_hbm, tokens, token_sem)
    token_copy.start()
    token_copy.wait()
    first_copies = []
    for k in range(mp):
        m = flip(col, k)
        copy = pltpu.make_async_copy(
            w_in_hbm.at[0, rows_of(m, narrow), :], first.at[m], first_sem.at[k]
        )
        copy.start()
        first_copies.append(copy)
    total = jnp.zeros((experts * SLOTS, narrow), jnp.float32)
    for group in range(GROUPS):
        code = places(
            index_ref[pl.ds(group, 1), :], slot_ref[pl.ds(group, 1), :],
            kept_ref[pl.ds(group, 1), :], group,
        )
        rows = lax.broadcasted_iota(jnp.int32, (experts * SLOTS, code.shape[1]), 0)
        table = jnp.where(rows == code, 1.0, 0.0).astype(jnp.bfloat16)
        total = total + jnp.dot(table, tokens[group], preferred_element_type=jnp.float32)
    packed[...] = total.astype(jnp.bfloat16)

    pl.semaphore_wait(barrier, experts + mp - 2)

    def exchange(j):
        e = flip(me, j)
        return remote(
            packed.at[rows_of(e, SLOTS), :], inbox.at[rows_of(me, SLOTS), :],
            a_send.at[j], a_recv.at[j], e, col,
        )

    def exchange_arrival(j):
        e = flip(me, j)
        return remote(
            packed.at[rows_of(e, SLOTS), :], inbox.at[rows_of(e, SLOTS), :],
            a_send.at[j], a_recv.at[j], e, col,
        )

    for j in range(experts - 1, 0, -1):
        exchange(j).start()
    out_order = list(range(mp - 1, -1, -1))
    second_copies = {}
    for k in out_order:
        m = flip(col, k)
        copy = pltpu.make_async_copy(
            w_out_hbm.at[0, :, rows_of(m, narrow)], second.at[m], second_sem.at[k]
        )
        copy.start()
        second_copies[k] = copy
    inbox[rows_of(me, SLOTS), :] = packed[rows_of(me, SLOTS), :]

    def gather(k, h, owner):
        block = gathered.at[owner, rows_of(flip(mine, h), slim), :]
        return remote(block, block, g_send.at[k, h], g_recv.at[k, h], me, flip(col, k))

    def spread(h):
        for j in range(h * each, (h + 1) * each):
            if j > 0:
                exchange_arrival(j).wait_recv()
        half = flip(mine, h)
        table = compact_table(slim, span, False)
        gathered[col, rows_of(half, slim), :] = jnp.dot(
            table, inbox[rows_of(half, span), :], preferred_element_type=jnp.float32
        ).astype(jnp.bfloat16)
        for k in range(mp - 1, 0, -1):
            gather(k, h, col).start()

    def first_product(h, k):
        m = flip(col, k)
        if h == 0:
            first_copies[k].wait()
        if k > 0:
            gather(k, h, m).wait_recv()
        product = jnp.dot(
            gathered[m, rows_of(flip(mine, h), slim), :], first[m],
            preferred_element_type=jnp.float32,
        )
        if k == 0:
            pre[h] = product
        elif k < mp - 1:
            pre[h] += product
        else:
            hidden[...] = jnp.maximum(pre[h] + product, 0.0).astype(jnp.bfloat16)

    def scatter(k, h, sender):
        rows = rows_of(flip(mine, h), slim)
        return remote(
            partial.at[flip(col, k), rows, :], arrived.at[sender, rows, :],
            r_send.at[k, h], r_recv.at[k, h], me, flip(col, k),
        )

    def second_products(h):
        for k in out_order:
            m = flip(col, k)
            if h == 0:
                second_copies[k].wait()
            partial[m, rows_of(flip(mine, h), slim), :] = jnp.dot(
                hidden[...], second[m], preferred_element_type=jnp.float32
            ).astype(jnp.bfloat16)
            if k > 0:
                scatter(k, h, col).start()

    for h in range(HALVES):
        spread(h)
        first_product(h, 0)
    for h in range(HALVES):
        for k in range(1, mp):
            first_product(h, k)
        second_products(h)

    def give_back(j):
        e = flip(me, j)
        return remote(
            outgoing.at[rows_of(e, SLOTS), :], returned.at[rows_of(me, SLOTS), :],
            b_send.at[j], b_recv.at[j], e, col,
        )

    def give_back_arrival(j):
        e = flip(me, j)
        return remote(
            outgoing.at[rows_of(e, SLOTS), :], returned.at[rows_of(e, SLOTS), :],
            b_send.at[j], b_recv.at[j], e, col,
        )

    for h in range(HALVES):
        half = flip(mine, h)
        rows = rows_of(half, slim)
        summed = partial[col, rows, :].astype(jnp.float32)
        for k in range(1, mp):
            m = flip(col, k)
            scatter(k, h, m).wait_recv()
            summed = summed + arrived[m, rows, :].astype(jnp.float32)
        table = compact_table(slim, span, True)
        outgoing[rows_of(half, span), :] = jnp.dot(
            table, summed.astype(jnp.bfloat16), preferred_element_type=jnp.float32
        ).astype(jnp.bfloat16)
        for j in range((h + 1) * each - 1, h * each - 1, -1):
            if j > 0:
                give_back(j).start()
    returned[rows_of(me, SLOTS), :] = outgoing[rows_of(me, SLOTS), :]
    for j in range(1, experts):
        give_back_arrival(j).wait_recv()
    result = pltpu.make_async_copy(returned, out_hbm, out_sem)
    result.start()
    for j in range(1, experts):
        exchange(j).wait_send()
        give_back(j).wait_send()
    for k in range(1, mp):
        for h in range(HALVES):
            gather(k, h, col).wait_send()
            scatter(k, h, col).wait_send()
    result.wait()


def combine_kernel(index_ref, slot_ref, kept_ref, gate_ref, returned_ref, out_ref):
    held = index_ref.shape[1]
    diagonal = lax.broadcasted_iota(jnp.int32, (held, held), 0) == lax.broadcasted_iota(
        jnp.int32, (held, held), 1
    )
    for group in range(GROUPS):
        code = places(
            index_ref[pl.ds(group, 1), :], slot_ref[pl.ds(group, 1), :],
            kept_ref[pl.ds(group, 1), :], group,
        ).astype(jnp.float32)
        code = jnp.sum(jnp.where(diagonal, code, 0.0), axis=1, keepdims=True)
        gate = jnp.sum(
            jnp.where(diagonal, gate_ref[pl.ds(group, 1), :], 0.0), axis=1, keepdims=True
        )
        lanes = lax.broadcasted_iota(jnp.int32, (held, returned_ref.shape[0]), 1)
        table = jnp.where(lanes == code.astype(jnp.int32), 1.0, 0.0).astype(jnp.bfloat16)
        picked = jnp.dot(table, returned_ref[...], preferred_element_type=jnp.float32)
        out_ref[group] = (gate * picked).astype(jnp.bfloat16)


def on_device(experts, mp, tokens, expert_index, slot_index, kept_mask, gate_prob, w_in, w_out):
    narrow = tokens.shape[2]
    width = w_in.shape[2]
    rows = experts * SLOTS
    slim = experts * USED
    vmem = pl.BlockSpec(memory_space=pltpu.VMEM)
    hbm = pl.BlockSpec(memory_space=pl.ANY)
    dma = pltpu.SemaphoreType.DMA
    bf16 = jnp.bfloat16
    returned = pl.pallas_call(
        functools.partial(expert_kernel, experts, mp),
        out_shape=jax.ShapeDtypeStruct((rows, narrow), bf16),
        in_specs=[vmem] * 3 + [hbm] * 3,
        out_specs=hbm,
        scratch_shapes=[
            pltpu.VMEM(tokens.shape, bf16),
            pltpu.VMEM((mp, narrow, width), bf16),
            pltpu.VMEM((mp, width, narrow), bf16),
            pltpu.VMEM((rows, narrow), bf16),
            pltpu.VMEM((rows, narrow), bf16),
            pltpu.VMEM((mp, slim, narrow), bf16),
            pltpu.VMEM((HALVES, slim // HALVES, width), jnp.float32),
            pltpu.VMEM((slim // HALVES, width), bf16),
            pltpu.VMEM((mp, slim, narrow), bf16),
            pltpu.VMEM((mp, slim, narrow), bf16),
            pltpu.VMEM((rows, narrow), bf16),
            pltpu.VMEM((rows, narrow), bf16),
            dma, dma((mp,)), dma((mp,)),
            dma((experts,)), dma((experts,)),
            dma((mp, HALVES)), dma((mp, HALVES)),
            dma((mp, HALVES)), dma((mp, HALVES)),
            dma((experts,)), dma((experts,)),
            dma,
        ],
        compiler_params=pltpu.CompilerParams(
            collective_id=0, has_side_effects=True, vmem_limit_bytes=60000 * 1024
        ),
    )(expert_index, slot_index, kept_mask, tokens, w_in, w_out)
    return pl.pallas_call(
        combine_kernel,
        out_shape=jax.ShapeDtypeStruct(tokens.shape, bf16),
        in_specs=[vmem] * 5,
        out_specs=vmem,
    )(expert_index, slot_index, kept_mask, gate_prob, returned)


def solution(mesh):
    placed = (
        P(None, "expert", "mp"),
        P(None, "expert"),
        P(None, "expert"),
        P(None, "expert"),
        P(None, "expert"),
        P("expert", None, "mp"),
        P("expert", "mp", None),
    )
    return jax.shard_map(
        functools.partial(on_device, mesh.shape["expert"], mesh.shape["mp"]),
        mesh=mesh, in_specs=placed, out_specs=P(None, "expert", "mp"), check_vma=False,
    )
```
